32 devices in a mesh: row: 8 (over z, core), col: 4 (over y, x).
Axes of the slice: x: 2, y: 2, z: 4, core: 2. Of those that a mesh axis runs over, the one named last changes fastest.
Arguments:
- matrix: float32 [1728, 65536], P('row', 'col'), may hold values from -6 to 6
- range_basis: float32 [1728, 384], P('col', 'row'), may hold values from -0.21875 to 0.21875
Outputs:
- projected: float32 [384, 65536], P('row')
The draws below stay inside these ranges and needn't reach their ends.
All inputs are finite; a program needn't handle non-finite values.
Results may differ from the reference program's by a relative error of at most 0.000071.
Values sent between devices are 32-bit elements; how exact they have to be, the bound alone decides.
A program may use at most 128 MiB of HBM per device.

```python
import jax
import jax.numpy as jnp
from jax import lax

K = 384
M = 1728
N = 65536


def spiked(entries, own_key, source, target, shards_of, factor):
    owner, partner = [(jnp.arange(entries.shape[axis_at]) // (entries.shape[axis_at] // shards_of)).reshape([-1 if axis == axis_at else 1 for axis in range(entries.ndim)]) for axis_at in (source, target)]
    chosen = jax.random.permutation(own_key, shards_of)[partner]
    strong = (owner == chosen) | (owner == (partner + shards_of // 2) % shards_of)
    return jnp.where(strong, factor * entries, entries)


def levels(rng, shape, pieces, least, high):
    gain = 1.0
    for dim, parts in pieces:
        draws = jax.random.uniform(jax.random.fold_in(jax.random.fold_in(rng, 6), dim), (parts,), jnp.float32, least / len(pieces), high / len(pieces))
        gain = gain * jnp.repeat(jnp.exp(draws), shape[dim] // parts).reshape((-1,) + (1,) * (len(shape) - 1 - dim))
    return gain


def centred(stream_key, dims, width, bound, shards=(), kind=jnp.bfloat16):
    array = width * jax.random.normal(stream_key, dims, jnp.float32)
    if shards:
        array = array * levels(stream_key, dims, shards, -0.22, 0.18)
    return jnp.clip(array, -bound, bound).astype(kind)


def gaussian_with(key, shape, scale, reach, cuts, heavy, dtype=jnp.bfloat16):
    result = scale * jax.random.normal(key, shape, jnp.float32)
    if cuts:
        result = result * levels(key, shape, cuts, -0.22, 0.18)
    return jnp.clip(spiked(result, jax.random.fold_in(key, 3), *heavy), -reach, reach).astype(dtype)


def setup_inputs(seed: int = 0) -> dict:
    arg_keys = jax.random.split(jax.random.key(seed), 3)
    matrix = centred(arg_keys[0], (M, N), 1.0, 6.0, ((0, 8), (1, 4)), jnp.float32)
    range_basis = gaussian_with(arg_keys[1], (M, K), M ** -0.5, 0.21875, ((0, 4), (1, 8)), (0, 1, 8, 2.0), jnp.float32)
    return {"matrix": matrix, "range_basis": range_basis}


def reference(matrix, range_basis):
    return lax.dot_general(range_basis, matrix, (((0,), (0,)), ((), ())), precision=lax.Precision.HIGHEST, preferred_element_type=jnp.float32)
```

```python
import functools

import jax
import jax.numpy as jnp
from jax import lax
from jax.experimental import pallas as pl
from jax.experimental.pallas import tpu as pltpu
from jax.sharding import PartitionSpec as P

MESH = pl.DeviceIdType.MESH
CORES = 2
WIDTH = 512
LEAD = 4
SKEW = 1
SPARE = 3
AHEAD = 3


def split_parts(value):
    high = value.astype(jnp.bfloat16)
    return high, (value - high.astype(jnp.float32)).astype(jnp.bfloat16)


def dot(left, right):
    return jnp.dot(left, right, preferred_element_type=jnp.float32)


def kernel(
    chips, cols, basis_ref, matrix_ref, out_ref, mine_basis, basis, halves, rows, part, sums,
    basis_load, basis_send, basis_recv, rows_local, rows_send, rows_recv,
    sum_send, sum_recv, out_send, out_recv,
):
    row, col = lax.axis_index("row"), lax.axis_index("col")
    chip, core = row // CORES, row % CORES
    vectors, inner = basis_ref.shape
    depth, block = matrix_ref.shape
    steps, _, width = rows.shape
    count = chips * vectors
    tile = min(256, width)
    first, last = chip == 0, chip == chips - 1
    ends = first | last
    ring = part.shape[0]

    def device(at_chip, at_col, at_core=core):
        return {"row": CORES * at_chip + at_core, "col": at_col}

    def basis_copy(target):
        return pltpu.make_async_remote_copy(
            src_ref=mine_basis,
            dst_ref=basis.at[chip],
            send_sem=basis_send.at[target],
            recv_sem=basis_recv.at[chip],
            device_id=device(col, target),
            device_id_type=MESH,
        )

    def basis_own():
        return pltpu.make_async_copy(basis_ref, basis.at[chip], basis_recv.at[chip])

    def basis_wait(source):
        pltpu.make_async_copy(basis_ref, basis.at[source], basis_recv.at[source]).wait()

    def rows_own(step):
        return pltpu.make_async_copy(
            matrix_ref.at[:, pl.ds(step * width, width)],
            rows.at[step, pl.ds(core * depth, depth)],
            rows_local.at[step],
        )

    def rows_peer(step, owner):
        return pltpu.make_async_remote_copy(
            src_ref=matrix_ref.at[:, pl.ds(step * width, width)],
            dst_ref=rows.at[step, pl.ds(owner * depth, depth)],
            send_sem=rows_send.at[step],
            recv_sem=rows_recv.at[step],
            device_id=device(chip, col, 1 - core),
            device_id_type=MESH,
        )

    def sum_copy(source, owner, slot, step, towards):
        return pltpu.make_async_remote_copy(
            src_ref=source,
            dst_ref=sums.at[slot, step],
            send_sem=sum_send.at[owner, step],
            recv_sem=sum_recv.at[slot, step],
            device_id=device(towards, col),
            device_id_type=MESH,
        )

    def owned(owner):
        return pl.ds(pl.multiple_of(owner * vectors, vectors), vectors)

    def part_of(step, owner):
        return part.at[lax.rem(step, ring), owned(owner)]

    def send_up(source, owner, step):
        sum_copy(source, owner, owner, step, chip + 1).start()

    def send_down(source, owner, step):
        slot = jnp.where(owner == chip - 1, chips, owner)
        sum_copy(source, owner, slot, step, chip - 1).start()

    neighbour = jnp.where(first, 1, chip - 1)

    def sum_wait(slot, step):
        sum_copy(sums.at[slot, step], 0, slot, step, neighbour).wait_recv()

    def sums_sent(step):
        for owner in range(chips):

            @pl.when(owner != chip)
            def _():
                sum_copy(sums.at[owner, step], owner, owner, step, neighbour).wait_send()

    def out_at(step, owner):
        return out_ref.at[:, pl.ds(pl.multiple_of(owner * block + step * width, width), width)]

    def out_copy(step, target, owner):
        return pltpu.make_async_remote_copy(
            src_ref=out_at(step, col),
            dst_ref=out_at(step, owner),
            send_sem=out_send.at[target, step],
            recv_sem=out_recv.at[owner, step],
            device_id=device(chip, target),
            device_id_type=MESH,
        )

    load = pltpu.make_async_copy(basis_ref, mine_basis, basis_load)
    load.start()
    for step in range(AHEAD):
        rows_own(step).start()

    barrier = pltpu.get_barrier_semaphore()

    def greet(where):
        pl.semaphore_signal(barrier, inc=1, device_id=where, device_id_type=MESH)

    greet(device(chip, col, 1 - core))
    for source in range(chips):
        pl.when((source != chip) | (col != chip))(lambda: greet(device(source, chip)))
    pl.when(chip > 0)(lambda: greet(device(chip - 1, col)))
    pl.when(chip < chips - 1)(lambda: greet(device(chip + 1, col)))
    for shift in range(1, cols):
        greet(device(chip, lax.rem(col + shift, cols)))
    greeted = 1 + chips - jnp.where(col == chip, 1, 0) + 2 - jnp.where(ends, 1, 0) + cols - 1
    load.wait()
    pl.when(chip == col)(lambda: basis_own().start())
    pl.semaphore_wait(barrier, greeted)

    for shift in range(cols):
        target = lax.rem(col + shift, cols)
        if shift:
            basis_copy(target).start()
        else:
            pl.when(chip != col)(lambda: basis_copy(col).start())
    for step in range(AHEAD):
        rows_peer(step, core).start()

    def fetch(step):
        @pl.when(step < steps)
        def _():
            rows_own(step).start()
            rows_peer(step, core).start()

    def rows_ready(step):
        rows_own(step).wait()
        rows_peer(step, 1 - core).wait_recv()

    def tiles(body):
        @pl.loop(0, width // tile)
        def _(at):
            body(pl.ds(pl.multiple_of(at * tile, tile), tile))

    rows_ready(0)
    way = jnp.where(chip < chips // 2, 1, chips - 1)
    for hop in range(1, chips + 1):
        owner = lax.rem(chip + hop * way, chips)
        basis_wait(owner)

        @functools.partial(tiles)
        def _(lanes):
            right, rest = split_parts(rows[0, :, lanes])
            high, low = split_parts(basis[owner])
            part[0, owned(owner), lanes] = dot(high, right) + (dot(low, right) + dot(high, rest))

        if hop < chips:
            pl.when(first)(lambda: send_up(part_of(0, owner), owner, 0))
            pl.when(last)(lambda: send_down(part_of(0, owner), owner, 0))

    high, low = split_parts(basis[...].reshape(count, inner))
    halves[:count, :inner] = high
    halves[count:, :inner] = low

    def compute(step):
        fetch(step + AHEAD - 1)
        rows_ready(step)
        slot = lax.rem(step, ring)

        @pl.when(ends & (step >= ring))
        def _():
            sums_sent(step - ring)

        @functools.partial(tiles)
        def _(lanes):
            right, rest = split_parts(rows[step, :, lanes])
            both = dot(halves[:, :inner], right)
            third = dot(halves[:count, :inner], rest)
            part[slot, :, lanes] = both[:count] + (both[count:] + third)

    def launch(tick):
        for far in range(chips - 1):
            step = tick - SKEW * far

            @pl.when((step > 0) & (step < steps))
            def _():
                up, down = chips - 1 - far, far
                pl.when(first)(lambda: send_up(part_of(step, up), up, step))
                pl.when(last)(lambda: send_down(part_of(step, down), down, step))

    @pl.loop(1, LEAD)
    def _(step):
        compute(step)
        launch(step)

    def forward(owner, step, send):
        @pl.when((step >= 0) & (step < steps))
        def _():
            sum_wait(owner, step)
            sums[owner, step] = sums[owner, step] + part[lax.rem(step, ring), owned(owner)]
            send(sums.at[owner, step], owner, step)

    @pl.loop(0, steps + SKEW * (chips - 1))
    def _(turn):
        pl.when(turn + LEAD < steps)(lambda: compute(turn + LEAD))
        launch(turn + LEAD)

        for owner in range(chips - 1, 0, -1):
            step = turn - SKEW * (chip + chips - 1 - owner)
            pl.when((chip > 0) & (chip < owner))(lambda: forward(owner, step, send_up))
            down = chips - 1 - owner
            back = turn - SKEW * (chips - 1 - chip + down)
            pl.when((chip < chips - 1) & (chip > down))(lambda: forward(down, back, send_down))

        @pl.when(turn >= SKEW * (chips - 1))
        def _():
            step = turn - SKEW * (chips - 1)
            slot = lax.rem(step, ring)
            here = pl.ds(pl.multiple_of(col * block + step * width, width), width)

            @pl.when(first)
            def _():
                sum_wait(chips, step)
                out_ref[:, here] = sums[chips, step] + part[slot, owned(chip)]

            @pl.when(last)
            def _():
                sum_wait(chip, step)
                out_ref[:, here] = sums[chip, step] + part[slot, owned(chip)]

            @pl.when(jnp.logical_not(ends))
            def _():
                sum_wait(chip, step)
                sum_wait(chips, step)
                out_ref[:, here] = sums[chip, step] + (sums[chips, step] + part[slot, owned(chip)])

            for shift in range(1, cols):
                out_copy(step, lax.rem(col + shift, cols), col).start()

    for shift in range(cols):
        target = lax.rem(col + shift, cols)
        if shift:
            basis_copy(target).wait_send()
        else:
            pl.when(chip != col)(lambda: basis_copy(col).wait_send())

    @pl.loop(0, steps)
    def _(step):
        rows_peer(step, core).wait_send()
        pl.when(jnp.logical_not(ends) | (step >= steps - ring))(lambda: sums_sent(step))
        for shift in range(1, cols):
            other = lax.rem(col + shift, cols)
            out_copy(step, other, col).wait_send()
            out_copy(step, other, other).wait_recv()


def solution(mesh):
    chips, cols = mesh.shape["row"] // CORES, mesh.shape["col"]

    def per_device(matrix, range_basis):
        depth, block = matrix.shape
        inner, vectors = range_basis.shape
        assert chips == cols and inner == CORES * depth and block % WIDTH == 0
        steps = block // WIDTH
        ring = LEAD + SKEW * (chips - 1) + SPARE
        padded = -(-inner // 128) * 128
        count = chips * vectors
        dma = pltpu.SemaphoreType.DMA
        return pl.pallas_call(
            functools.partial(kernel, chips, cols),
            out_shape=pltpu.VMEM((vectors, cols * block), jnp.float32),
            in_specs=[pl.BlockSpec(memory_space=pl.ANY)] * 2,
            out_specs=pl.BlockSpec(memory_space=pltpu.VMEM),
            scratch_shapes=[
                pltpu.VMEM((vectors, inner), jnp.float32),
                pltpu.VMEM((chips, vectors, inner), jnp.float32),
                pltpu.VMEM((2 * count, padded), jnp.bfloat16),
                pltpu.VMEM((steps, inner, WIDTH), jnp.float32),
                pltpu.VMEM((ring, count, WIDTH), jnp.float32),
                pltpu.VMEM((chips + 1, steps, vectors, WIDTH), jnp.float32),
                dma,
                dma((cols,)),
                dma((chips,)),
                dma((steps,)),
                dma((steps,)),
                dma((steps,)),
                dma((chips, steps)),
                dma((chips + 1, steps)),
                dma((cols, steps)),
                dma((cols, steps)),
            ],
            compiler_params=pltpu.CompilerParams(
                has_side_effects=True, collective_id=0, vmem_limit_bytes=52_000_000
            ),
        )(range_basis.T, matrix)

    return jax.shard_map(
        per_device,
        mesh=mesh,
        in_specs=(P("row", "col"), P("col", "row")),
        out_specs=P("row", None),
        check_vma=False,
    )
```

```python
import functools

import jax
import jax.numpy as jnp
from jax import lax
from jax.experimental import pallas as pl
from jax.experimental.pallas import tpu as pltpu
from jax.sharding import PartitionSpec as P

MESH = pl.DeviceIdType.MESH
CORES = 2
WIDTH = 512
LEAD = 4
SKEW = 1
SPARE = 3
AHEAD = 6


def split_parts(value):
    high = value.astype(jnp.bfloat16)
    return high, (value - high.astype(jnp.float32)).astype(jnp.bfloat16)


def dot(left, right):
    return jnp.dot(left, right, preferred_element_type=jnp.float32)


def kernel(
    chips, cols, basis_ref, matrix_ref, out_ref, loaded, cut, relay, basis, halves, rows, part, sums,
    basis_load, cut_send, cut_recv, line_send, spread_send, basis_recv, rows_local, rows_send, rows_recv,
    sum_send, sum_recv, out_send, out_recv,
):
    row, col = lax.axis_index("row"), lax.axis_index("col")
    chip, core = row // CORES, row % CORES
    vectors, inner = basis_ref.shape
    depth, block = matrix_ref.shape
    steps, _, width = rows.shape
    count = chips * vectors
    tile = min(256, width)
    first, last = chip == 0, chip == chips - 1
    ends = first | last
    ring = part.shape[0]

    def device(at_chip, at_col, at_core=core):
        return {"row": CORES * at_chip + at_core, "col": at_col}

    cuts = cut.shape[0]

    def cut_copy(target):
        return pltpu.make_async_remote_copy(
            src_ref=cut.at[target],
            dst_ref=relay.at[col],
            send_sem=cut_send.at[target],
            recv_sem=cut_recv.at[col],
            device_id=device(chip, target),
            device_id_type=MESH,
        )

    def cut_wait(source):
        pltpu.make_async_copy(cut.at[0], relay.at[source], cut_recv.at[source]).wait()

    def line_copy(plane):
        return pltpu.make_async_remote_copy(
            src_ref=relay.at[plane],
            dst_ref=basis.at[chip, col],
            send_sem=line_send.at[plane],
            recv_sem=basis_recv.at[chip, col],
            device_id=device(plane, col),
            device_id_type=MESH,
        )

    def spread_copy(source, owner, target):
        return pltpu.make_async_remote_copy(
            src_ref=source,
            dst_ref=basis.at[owner, col],
            send_sem=spread_send.at[owner, target],
            recv_sem=basis_recv.at[owner, col],
            device_id=device(chip, target),
            device_id_type=MESH,
        )

    def basis_wait(owner, at):
        pltpu.make_async_copy(cut.at[0], basis.at[owner, at], basis_recv.at[owner, at]).wait()

    def rows_own(step):
        return pltpu.make_async_copy(
            matrix_ref.at[:, pl.ds(step * width, width)],
            rows.at[step, pl.ds(core * depth, depth)],
            rows_local.at[step],
        )

    def rows_peer(step, owner):
        return pltpu.make_async_remote_copy(
            src_ref=matrix_ref.at[:, pl.ds(step * width, width)],
            dst_ref=rows.at[step, pl.ds(owner * depth, depth)],
            send_sem=rows_send.at[step],
            recv_sem=rows_recv.at[step],
            device_id=device(chip, col, 1 - core),
            device_id_type=MESH,
        )

    def sum_copy(source, owner, slot, step, towards):
        return pltpu.make_async_remote_copy(
            src_ref=source,
            dst_ref=sums.at[slot, step],
            send_sem=sum_send.at[owner, step],
            recv_sem=sum_recv.at[slot, step],
            device_id=device(towards, col),
            device_id_type=MESH,
        )

    def owned(owner):
        return pl.ds(pl.multiple_of(owner * vectors, vectors), vectors)

    def part_of(step, owner):
        return part.at[lax.rem(step, ring), owned(owner)]

    def send_up(source, owner, step):
        sum_copy(source, owner, owner, step, chip + 1).start()

    def send_down(source, owner, step):
        slot = jnp.where(owner == chip - 1, chips, owner)
        sum_copy(source, owner, slot, step, chip - 1).start()

    neighbour = jnp.where(first, 1, chip - 1)

    def sum_wait(slot, step):
        sum_copy(sums.at[slot, step], 0, slot, step, neighbour).wait_recv()

    def sums_sent(step):
        for owner in range(chips):

            @pl.when(owner != chip)
            def _():
                sum_copy(sums.at[owner, step], owner, owner, step, neighbour).wait_send()

    def out_at(step, owner):
        return out_ref.at[:, pl.ds(pl.multiple_of(owner * block + step * width, width), width)]

    def out_copy(step, target, owner):
        return pltpu.make_async_remote_copy(
            src_ref=out_at(step, col),
            dst_ref=out_at(step, owner),
            send_sem=out_send.at[target, step],
            recv_sem=out_recv.at[owner, step],
            device_id=device(chip, target),
            device_id_type=MESH,
        )

    load = pltpu.make_async_copy(basis_ref, loaded, basis_load)
    load.start()
    for step in range(AHEAD):
        rows_own(step).start()

    barrier = pltpu.get_barrier_semaphore()

    def greet(where):
        pl.semaphore_signal(barrier, inc=1, device_id=where, device_id_type=MESH)

    for plane in range(chips):
        pl.when(plane != chip)(lambda: greet(device(plane, col)))
    for shift in range(1, cols):
        greet(device(chip, lax.rem(col + shift, cols)))
    greet(device(chip, col, 1 - core))
    load.wait()
    for at in range(cuts):
        size = min(128, inner - at * 128)
        cut[at, :, :size] = loaded[:, at * 128 : at * 128 + size]
        if size < 128:
            cut[at, :, size:] = jnp.zeros((vectors, 128 - size), jnp.float32)

    relays = col < cuts

    @pl.when(relays)
    def _():
        relay[col] = cut[lax.rem(col, cuts)]

    pl.semaphore_wait(barrier, chips + cols - 1)

    for shift in range(1, cols):
        target = lax.rem(col + shift, cols)
        pl.when(target < cuts)(lambda: cut_copy(target).start())
    rows_peer(0, core).start()

    low_half = chip < chips // 2
    way = jnp.where(low_half, 1, chips - 1)

    @pl.when(relays)
    def _():
        for hop in range(chips):
            plane = jnp.where(low_half, hop, chips - 1 - hop)
            pl.when(plane != col)(lambda: cut_wait(plane))
            pl.when(plane != chip)(lambda: line_copy(plane).start())

    rows_peer(1, core).start()

    @pl.when(relays)
    def _():
        for hop in range(1, chips + 1):
            owner = lax.rem(chip + hop * way, chips)
            if hop < chips:
                basis_wait(owner, col)
            else:
                basis[owner, col] = relay[owner]
            source = basis.at[owner, col] if hop < chips else relay.at[owner]
            for shift in range(1, cols):
                spread_copy(source, owner, lax.rem(col + shift, cols)).start()

    for step in range(2, AHEAD):
        rows_peer(step, core).start()

    def fetch(step):
        @pl.when(step < steps)
        def _():
            rows_own(step).start()
            rows_peer(step, core).start()

    def rows_ready(step):
        rows_own(step).wait()
        rows_peer(step, 1 - core).wait_recv()

    def tiles(body):
        @pl.loop(0, width // tile)
        def _(at):
            body(pl.ds(pl.multiple_of(at * tile, tile), tile))

    for hop in range(1, chips + 1):
        owner = lax.rem(chip + hop * way, chips)
        for at in range(cuts):
            pl.when(col != at)(lambda: basis_wait(owner, at))

        @pl.loop(0, LEAD)
        def _(step):
            if hop == 1:
                rows_ready(step)

            @functools.partial(tiles)
            def _(lanes):
                right, rest = split_parts(rows[step, :, lanes])
                mine = jnp.concatenate([basis[owner, at] for at in range(cuts)], axis=1)
                high, low = split_parts(mine[:, :inner])
                part[step, owned(owner), lanes] = dot(high, right) + (dot(low, right) + dot(high, rest))

            if hop < chips:
                pl.when(first)(lambda: send_up(part_of(step, owner), owner, step))
                pl.when(last)(lambda: send_down(part_of(step, owner), owner, step))

    whole = [basis[:, at].reshape(count, 128) for at in range(cuts)]
    high, low = split_parts(jnp.concatenate(whole, axis=1))
    halves[:count] = high
    halves[count:] = low

    def compute(step):
        fetch(step + AHEAD - LEAD)
        rows_ready(step)
        slot = lax.rem(step, ring)

        @pl.when(ends & (step >= ring))
        def _():
            sums_sent(step - ring)

        @functools.partial(tiles)
        def _(lanes):
            right, rest = split_parts(rows[step, :, lanes])
            both = dot(halves[:, :inner], right)
            third = dot(halves[:count, :inner], rest)
            part[slot, :, lanes] = both[:count] + (both[count:] + third)

    def launch(tick):
        for far in range(chips - 1):
            step = tick - SKEW * far

            @pl.when((step >= LEAD) & (step < steps))
            def _():
                up, down = chips - 1 - far, far
                pl.when(first)(lambda: send_up(part_of(step, up), up, step))
                pl.when(last)(lambda: send_down(part_of(step, down), down, step))

    def forward(owner, step, send):
        @pl.when((step >= 0) & (step < steps))
        def _():
            sum_wait(owner, step)
            sums[owner, step] = sums[owner, step] + part[lax.rem(step, ring), owned(owner)]
            send(sums.at[owner, step], owner, step)

    @pl.loop(0, steps + SKEW * (chips - 1))
    def _(turn):
        pl.when(turn + LEAD < steps)(lambda: compute(turn + LEAD))
        launch(turn + LEAD)

        for owner in range(chips - 1, 0, -1):
            step = turn - SKEW * (chip + chips - 1 - owner)
            pl.when((chip > 0) & (chip < owner))(lambda: forward(owner, step, send_up))
            down = chips - 1 - owner
            back = turn - SKEW * (chips - 1 - chip + down)
            pl.when((chip < chips - 1) & (chip > down))(lambda: forward(down, back, send_down))

        @pl.when(turn >= SKEW * (chips - 1))
        def _():
            step = turn - SKEW * (chips - 1)
            slot = lax.rem(step, ring)
            here = pl.ds(pl.multiple_of(col * block + step * width, width), width)

            @pl.when(first)
            def _():
                sum_wait(chips, step)
                out_ref[:, here] = sums[chips, step] + part[slot, owned(chip)]

            @pl.when(last)
            def _():
                sum_wait(chip, step)
                out_ref[:, here] = sums[chip, step] + part[slot, owned(chip)]

            @pl.when(jnp.logical_not(ends))
            def _():
                sum_wait(chip, step)
                sum_wait(chips, step)
                out_ref[:, here] = sums[chip, step] + (sums[chips, step] + part[slot, owned(chip)])

            for shift in range(1, cols):
                out_copy(step, lax.rem(col + shift, cols), col).start()

    for shift in range(1, cols):
        target = lax.rem(col + shift, cols)
        pl.when(target < cuts)(lambda: cut_copy(target).wait_send())

    @pl.when(relays)
    def _():
        for plane in range(chips):
            pl.when(plane != chip)(lambda: line_copy(plane).wait_send())
            for shift in range(1, cols):
                spread_copy(relay.at[plane], plane, lax.rem(col + shift, cols)).wait_send()

    @pl.loop(0, steps)
    def _(step):
        rows_peer(step, core).wait_send()
        pl.when(jnp.logical_not(ends) | (step >= steps - ring))(lambda: sums_sent(step))
        for shift in range(1, cols):
            other = lax.rem(col + shift, cols)
            out_copy(step, other, col).wait_send()
            out_copy(step, other, other).wait_recv()


def solution(mesh):
    chips, cols = mesh.shape["row"] // CORES, mesh.shape["col"]

    def per_device(matrix, range_basis):
        depth, block = matrix.shape
        inner, vectors = range_basis.shape
        assert chips == cols >= -(-inner // 128) and inner == CORES * depth and block % WIDTH == 0
        steps = block // WIDTH
        ring = LEAD + SKEW * (chips - 1) + SPARE
        cuts = -(-inner // 128)
        padded = cuts * 128
        count = chips * vectors
        dma = pltpu.SemaphoreType.DMA
        return pl.pallas_call(
            functools.partial(kernel, chips, cols),
            out_shape=pltpu.VMEM((vectors, cols * block), jnp.float32),
            in_specs=[pl.BlockSpec(memory_space=pl.ANY)] * 2,
            out_specs=pl.BlockSpec(memory_space=pltpu.VMEM),
            scratch_shapes=[
                pltpu.VMEM((vectors, inner), jnp.float32),
                pltpu.VMEM((cuts, vectors, 128), jnp.float32),
                pltpu.VMEM((cols, vectors, 128), jnp.float32),
                pltpu.VMEM((chips, cuts, vectors, 128), jnp.float32),
                pltpu.VMEM((2 * count, padded), jnp.bfloat16),
                pltpu.VMEM((steps, inner, WIDTH), jnp.float32),
                pltpu.VMEM((ring, count, WIDTH), jnp.float32),
                pltpu.VMEM((chips + 1, steps, vectors, WIDTH), jnp.float32),
                dma,
                dma((cuts,)),
                dma((cols,)),
                dma((chips,)),
                dma((chips, cols)),
                dma((chips, cuts)),
                dma((steps,)),
                dma((steps,)),
                dma((steps,)),
                dma((chips, steps)),
                dma((chips + 1, steps)),
                dma((cols, steps)),
                dma((cols, steps)),
            ],
            compiler_params=pltpu.CompilerParams(
                has_side_effects=True, collective_id=0, vmem_limit_bytes=52_000_000
            ),
        )(range_basis.T, matrix)

    return jax.shard_map(
        per_device,
        mesh=mesh,
        in_specs=(P("row", "col"), P("col", "row")),
        out_specs=P("row", None),
        check_vma=False,
    )
```

```python
import functools

import jax
import jax.numpy as jnp
from jax import lax
from jax.experimental import pallas as pl
from jax.experimental.pallas import tpu as pltpu
from jax.sharding import PartitionSpec as P

MESH = pl.DeviceIdType.MESH
CORES = 2
WIDE = 1024
NARROW = 256
TILE = 512
TAPER = 2
LEAD = 2
SKEW = 1
SPARE = 1
AHEAD = 3


def split_parts(value):
    high = value.astype(jnp.bfloat16)
    return high, (value - high.astype(jnp.float32)).astype(jnp.bfloat16)


def dot(left, right):
    return jnp.dot(left, right, preferred_element_type=jnp.float32)


def kernel(
    chips, cols, basis_ref, matrix_ref, out_ref, loaded, cut, relay, basis, halves, rows, part, sums,
    lent_rows, lent_basis, lent_halves,
    basis_load, cut_send, cut_recv, line_send, spread_send, basis_recv, rows_local, rows_send, rows_recv,
    lent_send, lent_recv, lent_pass, lent_line, lent_spread, lent_basis_recv, sum_send, sum_recv, out_send, out_recv,
):
    row, col = lax.axis_index("row"), lax.axis_index("col")
    chip, core = row // CORES, row % CORES
    vectors, inner = basis_ref.shape
    depth, block = matrix_ref.shape
    count = chips * vectors
    wide = block // WIDE - TAPER
    steps = wide + TAPER * WIDE // NARROW
    first, last = chip == 0, chip == chips - 1
    ends = first | last
    ring = part.shape[0]
    lent = wide
    upper = chips - 2
    borrower = (chip == 1) | (chip == upper)
    lender = jnp.where(chip == 1, 0, chips - 1)

    def columns(step, size, base=0):
        start = jnp.where(step < wide, step * WIDE, wide * WIDE + (step - wide) * NARROW)
        return pl.ds(pl.multiple_of(base + start, NARROW), size)

    def sized(step, run):
        pl.when(step < wide)(lambda: run(WIDE))
        pl.when(step >= wide)(lambda: run(NARROW))

    def device(at_chip, at_col, at_core=core):
        return {"row": CORES * at_chip + at_core, "col": at_col}

    cuts = cut.shape[0]

    def cut_copy(target):
        return pltpu.make_async_remote_copy(
            src_ref=cut.at[target],
            dst_ref=relay.at[col],
            send_sem=cut_send.at[target],
            recv_sem=cut_recv.at[col],
            device_id=device(chip, target),
            device_id_type=MESH,
        )

    def cut_wait(source):
        pltpu.make_async_copy(cut.at[0], relay.at[source], cut_recv.at[source]).wait()

    def line_copy(plane):
        return pltpu.make_async_remote_copy(
            src_ref=relay.at[plane],
            dst_ref=basis.at[chip, col],
            send_sem=line_send.at[plane],
            recv_sem=basis_recv.at[chip, col],
            device_id=device(plane, col),
            device_id_type=MESH,
        )

    def spread_copy(source, owner, target):
        return pltpu.make_async_remote_copy(
            src_ref=source,
            dst_ref=basis.at[owner, col],
            send_sem=spread_send.at[owner, target],
            recv_sem=basis_recv.at[owner, col],
            device_id=device(chip, target),
            device_id_type=MESH,
        )

    def basis_wait(owner, at):
        pltpu.make_async_copy(cut.at[0], basis.at[owner, at], basis_recv.at[owner, at]).wait()

    def rows_own(step, size):
        return pltpu.make_async_copy(
            matrix_ref.at[:, columns(step, size)],
            rows.at[pl.ds(core * depth, depth), columns(step, size)],
            rows_local.at[step],
        )

    def rows_peer(step, size, owner):
        return pltpu.make_async_remote_copy(
            src_ref=matrix_ref.at[:, columns(step, size)],
            dst_ref=rows.at[pl.ds(owner * depth, depth), columns(step, size)],
            send_sem=rows_send.at[step],
            recv_sem=rows_recv.at[step],
            device_id=device(chip, col, 1 - core),
            device_id_type=MESH,
        )

    def lend():
        return pltpu.make_async_remote_copy(
            src_ref=matrix_ref.at[:, columns(lent, NARROW)],
            dst_ref=lent_rows.at[pl.ds(core * depth, depth)],
            send_sem=lent_send,
            recv_sem=lent_recv.at[core],
            device_id=device(jnp.where(first, 1, upper), col),
            device_id_type=MESH,
        )

    def lend_peer(owner):
        return pltpu.make_async_remote_copy(
            src_ref=lent_rows.at[pl.ds(core * depth, depth)],
            dst_ref=lent_rows.at[pl.ds(owner * depth, depth)],
            send_sem=lent_pass,
            recv_sem=lent_recv.at[owner],
            device_id=device(chip, col, 1 - core),
            device_id_type=MESH,
        )

    def lent_line_copy(plane, towards):
        return pltpu.make_async_remote_copy(
            src_ref=relay.at[plane],
            dst_ref=lent_basis.at[chip, col],
            send_sem=lent_line.at[min(plane, 1)],
            recv_sem=lent_basis_recv.at[chip, col],
            device_id=device(towards, col),
            device_id_type=MESH,
        )

    def lent_spread_copy(source, owner, target):
        return pltpu.make_async_remote_copy(
            src_ref=source,
            dst_ref=lent_basis.at[owner, col],
            send_sem=lent_spread.at[owner, target],
            recv_sem=lent_basis_recv.at[owner, col],
            device_id=device(chip, target),
            device_id_type=MESH,
        )

    def lent_wait(owner, at):
        pltpu.make_async_copy(cut.at[0], lent_basis.at[owner, at], lent_basis_recv.at[owner, at]).wait()

    def sum_at(slot, step, size):
        return sums.at[slot, :, columns(step, size)]

    def sum_copy(source, owner, slot, step, size, towards):
        return pltpu.make_async_remote_copy(
            src_ref=source,
            dst_ref=sum_at(slot, step, size),
            send_sem=sum_send.at[owner, step],
            recv_sem=sum_recv.at[slot, step],
            device_id=device(towards, col),
            device_id_type=MESH,
        )

    def owned(owner):
        return pl.ds(pl.multiple_of(owner * vectors, vectors), vectors)

    def part_of(step, size, owner):
        return part.at[lax.rem(step, ring), owned(owner), pl.ds(0, size)]

    def send_up(source, owner, step, size):
        sum_copy(source, owner, owner, step, size, chip + 1).start()

    def send_down(source, owner, step, size):
        slot = jnp.where(owner == chip - 1, chips, owner)
        sum_copy(source, owner, slot, step, size, chip - 1).start()

    neighbour = jnp.where(first, 1, chip - 1)

    def sum_wait(slot, step, size):
        sum_copy(sum_at(slot, step, size), 0, slot, step, size, neighbour).wait_recv()

    def sums_sent(step, size):
        for owner in range(chips):

            @pl.when(owner != chip)
            def _():
                sum_copy(sum_at(owner, step, size), owner, owner, step, size, neighbour).wait_send()

    def out_at(step, size, owner):
        return out_ref.at[:, columns(step, size, owner * block)]

    def out_copy(step, size, target, owner):
        return pltpu.make_async_remote_copy(
            src_ref=out_at(step, size, col),
            dst_ref=out_at(step, size, owner),
            send_sem=out_send.at[target, step],
            recv_sem=out_recv.at[owner, step],
            device_id=device(chip, target),
            device_id_type=MESH,
        )

    load = pltpu.make_async_copy(basis_ref, loaded, basis_load)
    load.start()
    for step in range(AHEAD):
        rows_own(step, WIDE).start()

    barrier = pltpu.get_barrier_semaphore()

    def greet(where):
        pl.semaphore_signal(barrier, inc=1, device_id=where, device_id_type=MESH)

    for plane in range(chips):
        pl.when(plane != chip)(lambda: greet(device(plane, col)))
    for shift in range(1, cols):
        greet(device(chip, lax.rem(col + shift, cols)))
    greet(device(chip, col, 1 - core))
    load.wait()
    for at in range(cuts):
        size = min(128, inner - at * 128)
        cut[at, :, :size] = loaded[:, at * 128 : at * 128 + size]
        if size < 128:
            cut[at, :, size:] = jnp.zeros((vectors, 128 - size), jnp.float32)

    relays = col < cuts

    @pl.when(relays)
    def _():
        relay[col] = cut[lax.rem(col, cuts)]

    pl.semaphore_wait(barrier, chips + cols - 1)

    for shift in range(1, cols):
        target = lax.rem(col + shift, cols)
        pl.when(target < cuts)(lambda: cut_copy(target).start())
    pl.when(ends)(lambda: lend().start())
    rows_peer(0, WIDE, core).start()

    low_half = chip < chips // 2
    way = jnp.where(low_half, 1, chips - 1)

    @pl.when(relays)
    def _():
        for hop in range(chips):
            plane = jnp.where(low_half, hop, chips - 1 - hop)
            pl.when(plane != col)(lambda: cut_wait(plane))
            pl.when(plane != chip)(lambda: line_copy(plane).start())

    rows_peer(1, WIDE, core).start()

    @pl.when(relays)
    def _():
        for hop in range(1, chips + 1):
            owner = lax.rem(chip + hop * way, chips)
            if hop < chips:
                basis_wait(owner, col)
            else:
                basis[owner, col] = relay[owner]
            source = basis.at[owner, col] if hop < chips else relay.at[owner]
            for shift in range(1, cols):
                spread_copy(source, owner, lax.rem(col + shift, cols)).start()

    loans = ((0, 1), (chips - 1, upper))

    @pl.when(relays)
    def _():
        for plane, towards in loans:
            pl.when((chip != plane) & (chip != towards))(lambda: lent_line_copy(plane, towards).start())

    for step in range(2, AHEAD):
        rows_peer(step, WIDE, core).start()

    def fetch(step):
        def run(size):
            rows_own(step, size).start()
            rows_peer(step, size, core).start()

        pl.when(step < steps)(lambda: sized(step, run))

    def rows_ready(step, size):
        rows_own(step, size).wait()
        rows_peer(step, size, 1 - core).wait_recv()

    def tiles(size, body):
        if size <= TILE:
            body(0)
        else:
            pl.loop(0, size // TILE)(lambda at: body(pl.multiple_of(at * TILE, TILE)))

    def product(left, right, size):
        value, rest = split_parts(right)
        both = dot(left[:, :inner], value)
        third = dot(left[:count, :inner], rest)
        return both[:count] + (both[count:] + third)

    for hop in range(1, chips + 1):
        owner = lax.rem(chip + hop * way, chips)
        for at in range(cuts):
            pl.when(col != at)(lambda: basis_wait(owner, at))

        @pl.loop(0, LEAD)
        def _(step):
            if hop == 1:
                rows_ready(step, WIDE)

            @functools.partial(tiles, WIDE)
            def _(at):
                right, rest = split_parts(rows[:, pl.ds(pl.multiple_of(step * WIDE + at, TILE), TILE)])
                mine = jnp.concatenate([basis[owner, at] for at in range(cuts)], axis=1)
                high, low = split_parts(mine[:, :inner])
                part[step, owned(owner), pl.ds(at, TILE)] = dot(high, right) + (dot(low, right) + dot(high, rest))

            if hop < chips:
                pl.when(first)(lambda: send_up(part_of(step, WIDE, owner), owner, step, WIDE))
                pl.when(last)(lambda: send_down(part_of(step, WIDE, owner), owner, step, WIDE))

    whole = [basis[:, at].reshape(count, 128) for at in range(cuts)]
    high, low = split_parts(jnp.concatenate(whole, axis=1))
    halves[:count] = high
    halves[count:] = low

    @pl.when(borrower)
    def _():
        lend_peer(core).wait_recv()
        lend_peer(core).start()

        @pl.when(relays)
        def _():
            lent_basis[chip, col] = relay[lender]
            for owner in range(chips):

                @pl.when(owner != lender)
                def _():
                    pl.when(owner != chip)(lambda: lent_wait(owner, col))
                    for shift in range(1, cols):
                        lent_spread_copy(lent_basis.at[owner, col], owner, lax.rem(col + shift, cols)).start()

        lent_basis[lender] = jnp.zeros((cuts, vectors, 128), jnp.float32)

    def compute(step, size):
        fetch(step + AHEAD - LEAD)
        rows_ready(step, size)
        slot = lax.rem(step, ring)
        old = step - ring

        @pl.when(ends & (old >= 0) & (old != lent))
        def _():
            sized(old, functools.partial(sums_sent, old))

        span = min(size, TILE)

        @functools.partial(tiles, size)
        def _(at):
            lanes = columns(step, span, at)
            part[slot, :, pl.ds(at, span)] = product(halves, rows[:, lanes], span)

        if size == NARROW:

            @pl.when(borrower & (step == lent))
            def _():
                for owner in range(chips):
                    for at in range(cuts):
                        pl.when((owner != lender) & (col != at))(lambda: lent_wait(owner, at))
                whole = [lent_basis[:, at].reshape(count, 128) for at in range(cuts)]
                high, low = split_parts(jnp.concatenate(whole, axis=1))
                lent_halves[:count] = high
                lent_halves[count:] = low
                lend_peer(1 - core).wait_recv()
                part[slot, :, pl.ds(0, size)] += product(lent_halves, lent_rows[...], size)

    def launch(tick):
        for far in range(chips - 1):
            step = tick - SKEW * far

            def run(size):
                up, down = chips - 1 - far, far
                pl.when(first)(lambda: send_up(part_of(step, size, up), up, step, size))
                pl.when(last)(lambda: send_down(part_of(step, size, down), down, step, size))

            @pl.when(ends & (step >= LEAD) & (step < steps) & (step != lent))
            def _():
                sized(step, run)

    def forward(owner, step, send, nearest):
        given = (step == lent) & (chip == nearest)

        def run(size):
            here = columns(step, size)

            @pl.when(given)
            def _():
                sums[owner, :, here] = part_of(step, size, owner)[...]

            @pl.when(jnp.logical_not(given))
            def _():
                sum_wait(owner, step, size)
                sums[owner, :, here] = sums[owner, :, here] + part_of(step, size, owner)[...]

            send(sum_at(owner, step, size), owner, step, size)

        pl.when((step >= 0) & (step < steps))(lambda: sized(step, run))

    def finish(step, size):
        total = part_of(step, size, chip)

        def add(slot):
            sum_wait(slot, step, size)
            total[...] += sums[slot, :, columns(step, size)]

        pl.when((chip > 0) & ((step != lent) | (chip != 1)))(lambda: add(chip))
        pl.when((chip < chips - 1) & ((step != lent) | (chip != upper)))(lambda: add(chips))
        out_ref[:, columns(step, size, col * block)] = total[...]
        for shift in range(1, cols):
            out_copy(step, size, lax.rem(col + shift, cols), col).start()

    @pl.loop(0, steps + SKEW * (chips - 1))
    def _(turn):
        ahead = turn + LEAD
        pl.when(ahead < steps)(lambda: sized(ahead, functools.partial(compute, ahead)))
        launch(ahead)

        for owner in range(chips - 1, 0, -1):
            step = turn - SKEW * (chip + chips - 1 - owner)
            pl.when((chip > 0) & (chip < owner))(lambda: forward(owner, step, send_up, 1))
            down = chips - 1 - owner
            back = turn - SKEW * (chips - 1 - chip + down)
            pl.when((chip < chips - 1) & (chip > down))(lambda: forward(down, back, send_down, upper))

        done = turn - SKEW * (chips - 1)
        pl.when(done >= 0)(lambda: sized(done, functools.partial(finish, done)))

    for shift in range(1, cols):
        target = lax.rem(col + shift, cols)
        pl.when(target < cuts)(lambda: cut_copy(target).wait_send())

    @pl.when(relays)
    def _():
        for plane in range(chips):
            pl.when(plane != chip)(lambda: line_copy(plane).wait_send())
            for shift in range(1, cols):
                spread_copy(relay.at[plane], plane, lax.rem(col + shift, cols)).wait_send()
        for plane, towards in loans:
            pl.when((chip != plane) & (chip != towards))(lambda: lent_line_copy(plane, towards).wait_send())

        @pl.when(borrower)
        def _():
            for owner in range(chips):
                for shift in range(1, cols):
                    target = lax.rem(col + shift, cols)
                    pl.when(owner != lender)(lambda: lent_spread_copy(relay.at[0], owner, target).wait_send())

    pl.when(ends)(lambda: lend().wait_send())
    pl.when(borrower)(lambda: lend_peer(core).wait_send())

    def drain(step, size):
        rows_peer(step, size, core).wait_send()
        left = jnp.logical_not(ends) | ((step >= steps - ring) & (step != lent))
        pl.when(left)(lambda: sums_sent(step, size))
        for shift in range(1, cols):
            other = lax.rem(col + shift, cols)
            out_copy(step, size, other, col).wait_send()
            out_copy(step, size, other, other).wait_recv()

    pl.loop(0, wide)(lambda step: drain(step, WIDE))
    pl.loop(wide, steps)(lambda step: drain(step, NARROW))


def solution(mesh):
    chips, cols = mesh.shape["row"] // CORES, mesh.shape["col"]

    def per_device(matrix, range_basis):
        depth, block = matrix.shape
        inner, vectors = range_basis.shape
        assert chips >= 4 and chips == cols >= -(-inner // 128) and inner == CORES * depth and block % WIDE == 0
        steps = block // WIDE - TAPER + TAPER * WIDE // NARROW
        ring = LEAD + SKEW * (chips - 1) + SPARE
        cuts = -(-inner // 128)
        padded = cuts * 128
        count = chips * vectors
        dma = pltpu.SemaphoreType.DMA
        return pl.pallas_call(
            functools.partial(kernel, chips, cols),
            out_shape=pltpu.VMEM((vectors, cols * block), jnp.float32),
            in_specs=[pl.BlockSpec(memory_space=pl.ANY)] * 2,
            out_specs=pl.BlockSpec(memory_space=pltpu.VMEM),
            scratch_shapes=[
                pltpu.VMEM((vectors, inner), jnp.float32),
                pltpu.VMEM((cuts, vectors, 128), jnp.float32),
                pltpu.VMEM((cols, vectors, 128), jnp.float32),
                pltpu.VMEM((chips, cuts, vectors, 128), jnp.float32),
                pltpu.VMEM((2 * count, padded), jnp.bfloat16),
                pltpu.VMEM((inner, block), jnp.float32),
                pltpu.VMEM((ring, count, WIDE), jnp.float32),
                pltpu.VMEM((chips + 1, vectors, block), jnp.float32),
                pltpu.VMEM((inner, NARROW), jnp.float32),
                pltpu.VMEM((chips, cuts, vectors, 128), jnp.float32),
                pltpu.VMEM((2 * count, padded), jnp.bfloat16),
                dma,
                dma((cuts,)),
                dma((cols,)),
                dma((chips,)),
                dma((chips, cols)),
                dma((chips, cuts)),
                dma((steps,)),
                dma((steps,)),
                dma((steps,)),
                dma,
                dma((CORES,)),
                dma,
                dma((2,)),
                dma((chips, cols)),
                dma((chips, cuts)),
                dma((chips, steps)),
                dma((chips + 1, steps)),
                dma((cols, steps)),
                dma((cols, steps)),
            ],
            compiler_params=pltpu.CompilerParams(
                has_side_effects=True, collective_id=0, vmem_limit_bytes=54_000_000
            ),
        )(range_basis.T, matrix)

    return jax.shard_map(
        per_device,
        mesh=mesh,
        in_specs=(P("row", "col"), P("col", "row")),
        out_specs=P("row", None),
        check_vma=False,
    )
```

```python
import functools

import jax
import jax.numpy as jnp
from jax import lax
from jax.experimental import pallas as pl
from jax.experimental.pallas import tpu as pltpu
from jax.sharding import PartitionSpec as P

MESH = pl.DeviceIdType.MESH
CORES = 2
WIDE = 1024
NARROW = 384
TILE = 512
TAPER = 3
LEAD = 2
SKEW = 1
SPARE = 1
AHEAD = 3


def split_parts(value):
    high = value.astype(jnp.bfloat16)
    return high, (value - high.astype(jnp.float32)).astype(jnp.bfloat16)


def dot(left, right):
    return jnp.dot(left, right, preferred_element_type=jnp.float32)


def kernel(
    chips, cols, basis_ref, matrix_ref, out_ref, loaded, cut, relay, basis, halves, rows, part, sums,
    lent_rows, lent_basis, lent_halves,
    basis_load, cut_send, cut_recv, line_send, spread_send, basis_recv, rows_local, rows_send, rows_recv,
    lent_send, lent_recv, lent_pass, lent_line, lent_spread, lent_basis_recv, sum_send, sum_recv, out_send, out_recv,
):
    row, col = lax.axis_index("row"), lax.axis_index("col")
    chip, core = row // CORES, row % CORES
    vectors, inner = basis_ref.shape
    depth, block = matrix_ref.shape
    count = chips * vectors
    wide = block // WIDE - TAPER
    steps = wide + TAPER * WIDE // NARROW
    first, last = chip == 0, chip == chips - 1
    ends = first | last
    ring = part.shape[0]
    lent = wide
    upper = chips - 2
    borrower = (chip == 1) | (chip == upper)
    lender = jnp.where(chip == 1, 0, chips - 1)

    def columns(step, size, base=0):
        start = jnp.where(step < wide, step * WIDE, wide * WIDE + (step - wide) * NARROW)
        return pl.ds(pl.multiple_of(base + start, 128), size)

    def sized(step, run):
        pl.when(step < wide)(lambda: run(WIDE))
        pl.when(step >= wide)(lambda: run(NARROW))

    def device(at_chip, at_col, at_core=core):
        return {"row": CORES * at_chip + at_core, "col": at_col}

    cuts = cut.shape[0]

    def cut_copy(target):
        return pltpu.make_async_remote_copy(
            src_ref=cut.at[target],
            dst_ref=relay.at[col],
            send_sem=cut_send.at[target],
            recv_sem=cut_recv.at[col],
            device_id=device(chip, target),
            device_id_type=MESH,
        )

    def cut_wait(source):
        pltpu.make_async_copy(cut.at[0], relay.at[source], cut_recv.at[source]).wait()

    def line_copy(plane):
        return pltpu.make_async_remote_copy(
            src_ref=relay.at[plane],
            dst_ref=basis.at[chip, col],
            send_sem=line_send.at[plane],
            recv_sem=basis_recv.at[chip, col],
            device_id=device(plane, col),
            device_id_type=MESH,
        )

    def spread_copy(source, owner, target):
        return pltpu.make_async_remote_copy(
            src_ref=source,
            dst_ref=basis.at[owner, col],
            send_sem=spread_send.at[owner, target],
            recv_sem=basis_recv.at[owner, col],
            device_id=device(chip, target),
            device_id_type=MESH,
        )

    def basis_wait(owner, at):
        pltpu.make_async_copy(cut.at[0], basis.at[owner, at], basis_recv.at[owner, at]).wait()

    def rows_own(step, size):
        return pltpu.make_async_copy(
            matrix_ref.at[:, columns(step, size)],
            rows.at[pl.ds(core * depth, depth), columns(step, size)],
            rows_local.at[step],
        )

    def rows_peer(step, size, owner):
        return pltpu.make_async_remote_copy(
            src_ref=matrix_ref.at[:, columns(step, size)],
            dst_ref=rows.at[pl.ds(owner * depth, depth), columns(step, size)],
            send_sem=rows_send.at[step],
            recv_sem=rows_recv.at[step],
            device_id=device(chip, col, 1 - core),
            device_id_type=MESH,
        )

    def lend():
        return pltpu.make_async_remote_copy(
            src_ref=matrix_ref.at[:, columns(lent, NARROW)],
            dst_ref=lent_rows.at[pl.ds(core * depth, depth)],
            send_sem=lent_send,
            recv_sem=lent_recv.at[core],
            device_id=device(jnp.where(first, 1, upper), col),
            device_id_type=MESH,
        )

    def lend_peer(owner):
        return pltpu.make_async_remote_copy(
            src_ref=lent_rows.at[pl.ds(core * depth, depth)],
            dst_ref=lent_rows.at[pl.ds(owner * depth, depth)],
            send_sem=lent_pass,
            recv_sem=lent_recv.at[owner],
            device_id=device(chip, col, 1 - core),
            device_id_type=MESH,
        )

    def lent_line_copy(plane, towards):
        return pltpu.make_async_remote_copy(
            src_ref=relay.at[plane],
            dst_ref=lent_basis.at[chip, col],
            send_sem=lent_line.at[min(plane, 1)],
            recv_sem=lent_basis_recv.at[chip, col],
            device_id=device(towards, col),
            device_id_type=MESH,
        )

    def lent_spread_copy(source, owner, target):
        return pltpu.make_async_remote_copy(
            src_ref=source,
            dst_ref=lent_basis.at[owner, col],
            send_sem=lent_spread.at[owner, target],
            recv_sem=lent_basis_recv.at[owner, col],
            device_id=device(chip, target),
            device_id_type=MESH,
        )

    def lent_wait(owner, at):
        pltpu.make_async_copy(cut.at[0], lent_basis.at[owner, at], lent_basis_recv.at[owner, at]).wait()

    def sum_at(slot, step, size):
        return sums.at[slot, :, columns(step, size)]

    def sum_copy(source, owner, slot, step, size, towards):
        return pltpu.make_async_remote_copy(
            src_ref=source,
            dst_ref=sum_at(slot, step, size),
            send_sem=sum_send.at[owner, step],
            recv_sem=sum_recv.at[slot, step],
            device_id=device(towards, col),
            device_id_type=MESH,
        )

    def owned(owner):
        return pl.ds(pl.multiple_of(owner * vectors, vectors), vectors)

    def part_of(step, size, owner):
        return part.at[lax.rem(step, ring), owned(owner), pl.ds(0, size)]

    def send_up(source, owner, step, size):
        sum_copy(source, owner, owner, step, size, chip + 1).start()

    def send_down(source, owner, step, size):
        slot = jnp.where(owner == chip - 1, chips, owner)
        sum_copy(source, owner, slot, step, size, chip - 1).start()

    neighbour = jnp.where(first, 1, chip - 1)

    def sum_wait(slot, step, size):
        sum_copy(sum_at(slot, step, size), 0, slot, step, size, neighbour).wait_recv()

    def sums_sent(step, size):
        for owner in range(chips):

            @pl.when(owner != chip)
            def _():
                sum_copy(sum_at(owner, step, size), owner, owner, step, size, neighbour).wait_send()

    def out_at(step, size, owner):
        return out_ref.at[:, columns(step, size, owner * block)]

    def out_copy(step, size, target, owner):
        return pltpu.make_async_remote_copy(
            src_ref=out_at(step, size, col),
            dst_ref=out_at(step, size, owner),
            send_sem=out_send.at[target, step],
            recv_sem=out_recv.at[owner, step],
            device_id=device(chip, target),
            device_id_type=MESH,
        )

    load = pltpu.make_async_copy(basis_ref, loaded, basis_load)
    load.start()
    for step in range(AHEAD):
        rows_own(step, WIDE).start()

    barrier = pltpu.get_barrier_semaphore()

    def greet(where):
        pl.semaphore_signal(barrier, inc=1, device_id=where, device_id_type=MESH)

    for plane in range(chips):
        pl.when(plane != chip)(lambda: greet(device(plane, col)))
    for shift in range(1, cols):
        greet(device(chip, lax.rem(col + shift, cols)))
    greet(device(chip, col, 1 - core))
    load.wait()
    for at in range(cuts):
        size = min(128, inner - at * 128)
        cut[at, :, :size] = loaded[:, at * 128 : at * 128 + size]
        if size < 128:
            cut[at, :, size:] = jnp.zeros((vectors, 128 - size), jnp.float32)

    relays = col < cuts

    @pl.when(relays)
    def _():
        relay[col] = cut[lax.rem(col, cuts)]

    pl.semaphore_wait(barrier, chips + cols - 1)

    for shift in range(1, cols):
        target = lax.rem(col + shift, cols)
        pl.when(target < cuts)(lambda: cut_copy(target).start())
    pl.when(ends)(lambda: lend().start())
    rows_peer(0, WIDE, core).start()

    low_half = chip < chips // 2
    way = jnp.where(low_half, 1, chips - 1)

    @pl.when(relays)
    def _():
        for hop in range(chips):
            plane = jnp.where(low_half, hop, chips - 1 - hop)
            pl.when(plane != col)(lambda: cut_wait(plane))
            pl.when(plane != chip)(lambda: line_copy(plane).start())

    rows_peer(1, WIDE, core).start()

    @pl.when(relays)
    def _():
        for hop in range(1, chips + 1):
            owner = lax.rem(chip + hop * way, chips)
            if hop < chips:
                basis_wait(owner, col)
            else:
                basis[owner, col] = relay[owner]
            source = basis.at[owner, col] if hop < chips else relay.at[owner]
            for shift in range(1, cols):
                spread_copy(source, owner, lax.rem(col + shift, cols)).start()

    loans = ((0, 1), (chips - 1, upper))

    @pl.when(relays)
    def _():
        for plane, towards in loans:
            pl.when((chip != plane) & (chip != towards))(lambda: lent_line_copy(plane, towards).start())

    for step in range(2, AHEAD):
        rows_peer(step, WIDE, core).start()

    def fetch(step):
        def run(size):
            rows_own(step, size).start()
            rows_peer(step, size, core).start()

        pl.when(step < steps)(lambda: sized(step, run))

    def rows_ready(step, size):
        rows_own(step, size).wait()
        rows_peer(step, size, 1 - core).wait_recv()

    def tiles(size, body):
        if size <= TILE:
            body(0)
        else:
            pl.loop(0, size // TILE)(lambda at: body(pl.multiple_of(at * TILE, TILE)))

    def product(left, right, size):
        value, rest = split_parts(right)
        both = dot(left[:, :inner], value)
        third = dot(left[:count, :inner], rest)
        return both[:count] + (both[count:] + third)

    for hop in range(1, chips + 1):
        owner = lax.rem(chip + hop * way, chips)
        for at in range(cuts):
            pl.when(col != at)(lambda: basis_wait(owner, at))

        @pl.loop(0, LEAD)
        def _(step):
            if hop == 1:
                rows_ready(step, WIDE)

            @functools.partial(tiles, WIDE)
            def _(at):
                right, rest = split_parts(rows[:, pl.ds(pl.multiple_of(step * WIDE + at, TILE), TILE)])
                mine = jnp.concatenate([basis[owner, at] for at in range(cuts)], axis=1)
                high, low = split_parts(mine[:, :inner])
                part[step, owned(owner), pl.ds(at, TILE)] = dot(high, right) + (dot(low, right) + dot(high, rest))

            if hop < chips:
                pl.when(first)(lambda: send_up(part_of(step, WIDE, owner), owner, step, WIDE))
                pl.when(last)(lambda: send_down(part_of(step, WIDE, owner), owner, step, WIDE))

    whole = [basis[:, at].reshape(count, 128) for at in range(cuts)]
    high, low = split_parts(jnp.concatenate(whole, axis=1))
    halves[:count] = high
    halves[count:] = low

    @pl.when(borrower)
    def _():
        lend_peer(core).wait_recv()
        lend_peer(core).start()

        @pl.when(relays)
        def _():
            lent_basis[chip, col] = relay[lender]
            for owner in range(chips):

                @pl.when(owner != lender)
                def _():
                    pl.when(owner != chip)(lambda: lent_wait(owner, col))
                    for shift in range(1, cols):
                        lent_spread_copy(lent_basis.at[owner, col], owner, lax.rem(col + shift, cols)).start()

        lent_basis[lender] = jnp.zeros((cuts, vectors, 128), jnp.float32)

    def compute(step, size):
        fetch(step + AHEAD - LEAD)
        rows_ready(step, size)
        slot = lax.rem(step, ring)
        old = step - ring

        @pl.when(ends & (old >= 0) & (old != lent))
        def _():
            sized(old, functools.partial(sums_sent, old))

        span = min(size, TILE)

        @functools.partial(tiles, size)
        def _(at):
            lanes = columns(step, span, at)
            part[slot, :, pl.ds(at, span)] = product(halves, rows[:, lanes], span)

        if size == NARROW:

            @pl.when(borrower & (step == lent))
            def _():
                for owner in range(chips):
                    for at in range(cuts):
                        pl.when((owner != lender) & (col != at))(lambda: lent_wait(owner, at))
                whole = [lent_basis[:, at].reshape(count, 128) for at in range(cuts)]
                high, low = split_parts(jnp.concatenate(whole, axis=1))
                lent_halves[:count] = high
                lent_halves[count:] = low
                lend_peer(1 - core).wait_recv()
                part[slot, :, pl.ds(0, size)] += product(lent_halves, lent_rows[...], size)

    def launch(tick):
        for far in range(chips - 1):
            step = tick - SKEW * far

            def run(size):
                up, down = chips - 1 - far, far
                pl.when(first)(lambda: send_up(part_of(step, size, up), up, step, size))
                pl.when(last)(lambda: send_down(part_of(step, size, down), down, step, size))

            @pl.when(ends & (step >= LEAD) & (step < steps) & (step != lent))
            def _():
                sized(step, run)

    def forward(owner, step, send, nearest):
        given = (step == lent) & (chip == nearest)

        def run(size):
            here = columns(step, size)

            @pl.when(given)
            def _():
                sums[owner, :, here] = part_of(step, size, owner)[...]

            @pl.when(jnp.logical_not(given))
            def _():
                sum_wait(owner, step, size)
                sums[owner, :, here] = sums[owner, :, here] + part_of(step, size, owner)[...]

            send(sum_at(owner, step, size), owner, step, size)

        pl.when((step >= 0) & (step < steps))(lambda: sized(step, run))

    def finish(step, size):
        total = part_of(step, size, chip)

        def add(slot):
            sum_wait(slot, step, size)
            total[...] += sums[slot, :, columns(step, size)]

        pl.when((chip > 0) & ((step != lent) | (chip != 1)))(lambda: add(chip))
        pl.when((chip < chips - 1) & ((step != lent) | (chip != upper)))(lambda: add(chips))
        out_ref[:, columns(step, size, col * block)] = total[...]
        for shift in range(1, cols):
            out_copy(step, size, lax.rem(col + shift, cols), col).start()

    @pl.loop(0, steps + SKEW * (chips - 1))
    def _(turn):
        ahead = turn + LEAD
        pl.when(ahead < steps)(lambda: sized(ahead, functools.partial(compute, ahead)))
        launch(ahead)

        for owner in range(chips - 1, 0, -1):
            step = turn - SKEW * (chip + chips - 1 - owner)
            pl.when((chip > 0) & (chip < owner))(lambda: forward(owner, step, send_up, 1))
            down = chips - 1 - owner
            back = turn - SKEW * (chips - 1 - chip + down)
            pl.when((chip < chips - 1) & (chip > down))(lambda: forward(down, back, send_down, upper))

        done = turn - SKEW * (chips - 1)
        pl.when(done >= 0)(lambda: sized(done, functools.partial(finish, done)))

    for shift in range(1, cols):
        target = lax.rem(col + shift, cols)
        pl.when(target < cuts)(lambda: cut_copy(target).wait_send())

    @pl.when(relays)
    def _():
        for plane in range(chips):
            pl.when(plane != chip)(lambda: line_copy(plane).wait_send())
            for shift in range(1, cols):
                spread_copy(relay.at[plane], plane, lax.rem(col + shift, cols)).wait_send()
        for plane, towards in loans:
            pl.when((chip != plane) & (chip != towards))(lambda: lent_line_copy(plane, towards).wait_send())

        @pl.when(borrower)
        def _():
            for owner in range(chips):
                for shift in range(1, cols):
                    target = lax.rem(col + shift, cols)
                    pl.when(owner != lender)(lambda: lent_spread_copy(relay.at[0], owner, target).wait_send())

    pl.when(ends)(lambda: lend().wait_send())
    pl.when(borrower)(lambda: lend_peer(core).wait_send())

    def drain(step, size):
        rows_peer(step, size, core).wait_send()
        left = jnp.logical_not(ends) | ((step >= steps - ring) & (step != lent))
        pl.when(left)(lambda: sums_sent(step, size))
        for shift in range(1, cols):
            other = lax.rem(col + shift, cols)
            out_copy(step, size, other, col).wait_send()
            out_copy(step, size, other, other).wait_recv()

    pl.loop(0, wide)(lambda step: drain(step, WIDE))
    pl.loop(wide, steps)(lambda step: drain(step, NARROW))


def solution(mesh):
    chips, cols = mesh.shape["row"] // CORES, mesh.shape["col"]

    def per_device(matrix, range_basis):
        depth, block = matrix.shape
        inner, vectors = range_basis.shape
        assert chips >= 4 and chips == cols >= -(-inner // 128) and inner == CORES * depth and block % WIDE == 0
        steps = block // WIDE - TAPER + TAPER * WIDE // NARROW
        ring = LEAD + SKEW * (chips - 1) + SPARE
        cuts = -(-inner // 128)
        padded = cuts * 128
        count = chips * vectors
        dma = pltpu.SemaphoreType.DMA
        return pl.pallas_call(
            functools.partial(kernel, chips, cols),
            out_shape=pltpu.VMEM((vectors, cols * block), jnp.float32),
            in_specs=[pl.BlockSpec(memory_space=pl.ANY)] * 2,
            out_specs=pl.BlockSpec(memory_space=pltpu.VMEM),
            scratch_shapes=[
                pltpu.VMEM((vectors, inner), jnp.float32),
                pltpu.VMEM((cuts, vectors, 128), jnp.float32),
                pltpu.VMEM((cols, vectors, 128), jnp.float32),
                pltpu.VMEM((chips, cuts, vectors, 128), jnp.float32),
                pltpu.VMEM((2 * count, padded), jnp.bfloat16),
                pltpu.VMEM((inner, block), jnp.float32),
                pltpu.VMEM((ring, count, WIDE), jnp.float32),
                pltpu.VMEM((chips + 1, vectors, block), jnp.float32),
                pltpu.VMEM((inner, NARROW), jnp.float32),
                pltpu.VMEM((chips, cuts, vectors, 128), jnp.float32),
                pltpu.VMEM((2 * count, padded), jnp.bfloat16),
                dma,
                dma((cuts,)),
                dma((cols,)),
                dma((chips,)),
                dma((chips, cols)),
                dma((chips, cuts)),
                dma((steps,)),
                dma((steps,)),
                dma((steps,)),
                dma,
                dma((CORES,)),
                dma,
                dma((2,)),
                dma((chips, cols)),
                dma((chips, cuts)),
                dma((chips, steps)),
                dma((chips + 1, steps)),
                dma((cols, steps)),
                dma((cols, steps)),
            ],
            compiler_params=pltpu.CompilerParams(
                has_side_effects=True, collective_id=0, vmem_limit_bytes=54_000_000
            ),
        )(range_basis.T, matrix)

    return jax.shard_map(
        per_device,
        mesh=mesh,
        in_specs=(P("row", "col"), P("col", "row")),
        out_specs=P("row", None),
        check_vma=False,
    )
```
